32 devices in a mesh: member: 4 (over z), lat: 4 (over y, core), lon: 2 (over x).
Axes of the slice: x: 2, y: 2, z: 4, core: 2. Of those that a mesh axis runs over, the one named last changes fastest.
Arguments:
- state: bfloat16 [100, 8, 720], P(None, 'lat', 'lon'), may hold values from -6 to 6
- target: bfloat16 [100, 8, 720], P(None, 'lat', 'lon'), may hold values from -6 to 6
- land_sea: int32 [8, 720], P('lat', 'lon'), may hold values 0 or 1
- seeds: int32 [4, 32], P('member'), may hold values from 0 to 65535
- w_in: bfloat16 [9, 100, 256], replicated, may hold values from -0.1875 to 0.1875
- w_mid: bfloat16 [9, 256, 256], replicated, may hold values from -0.125 to 0.125
- w_out: bfloat16 [100, 256], replicated, may hold values from -0.375 to 0.375
- w_noise: float32 [32, 256], replicated, may hold values from -1 to 1
Outputs:
- update_in: float32 [9, 100, 256], replicated
- update_mid: float32 [9, 256, 256], replicated
- update_out: float32 [100, 256], replicated
- update_noise: float32 [32, 256], replicated
- loss: float32 [], replicated
The draws below stay inside these ranges and needn't reach their ends.
All inputs are finite; a program needn't handle non-finite values. No bound on the sum of `land_sea` on one device may be relied on, other than what follows from the above.
Results may differ from the reference program's by a relative error of at most 0.0014.
Values may be sent and summed in bfloat16 or wider, within the bound.
A program may use at most 64 MiB of HBM per device.

```python
import jax
import jax.numpy as jnp
from jax import lax

V = 100
C = 256
NOISE = 32
MEMBERS = 4
NLAT = 8
NLON = 720


def with_ends(values, rng, least, largest):
    dims = values.shape
    index_at = [jax.random.randint(jax.random.fold_in(rng, axis), (), 0, dims[axis]) for axis in range(len(dims))]
    values = values.at[tuple(index_at)].set(least)
    longest = dims.index(max(dims))
    index_at[longest] = (index_at[longest] + 1) % dims[longest]
    return values.at[tuple(index_at)].set(largest)


def block_levels(key, extent, shards, low, top_value):
    gain = 1.0
    for dim, blocks in shards:
        heights = jax.random.uniform(jax.random.fold_in(jax.random.fold_in(key, 6), dim), (blocks,), jnp.float32, low / len(shards), top_value / len(shards))
        gain = gain * jnp.repeat(jnp.exp(heights), extent[dim] // blocks).reshape((-1,) + (1,) * (len(extent) - 1 - dim))
    return gain


def centred(own_key, dims, deviation, limit, pieces=(), dtype=jnp.bfloat16):
    array = deviation * jax.random.normal(own_key, dims, jnp.float32)
    if pieces:
        array = array * block_levels(own_key, dims, pieces, -0.22, 0.18)
    return jnp.clip(array, -limit, limit).astype(dtype)


def setup_inputs(seed: int = 0) -> dict:
    keys = jax.random.split(jax.random.key(seed), 9)
    return {
        "state": centred(keys[0], (V, NLAT, NLON), 1.0, 6.0, ((1, 4), (2, 2))),
        "target": centred(keys[1], (V, NLAT, NLON), 1.0, 6.0, ((1, 4), (2, 2))),
        "land_sea": with_ends((jax.random.randint(keys[2], (NLAT, NLON), 0, 10) < 3).astype(jnp.int32), jax.random.fold_in(keys[2], 1), 0, 1),
        "seeds": with_ends(jax.random.randint(keys[3], (MEMBERS, NOISE), 0, 65536), jax.random.fold_in(keys[3], 1), 0, 65535).astype(jnp.int32),
        "w_in": centred(keys[4], (9, V, C), (9 * V) ** -0.5, 0.1875),
        "w_mid": centred(keys[5], (9, C, C), (9 * C) ** -0.5, 0.125),
        "w_out": centred(keys[6], (V, C), C ** -0.5, 0.375),
        "w_noise": centred(keys[7], (NOISE, C), NOISE ** -0.5, 1.0, (), jnp.float32),
    }


SMOOTH = 0.25

def pad_grid(fields):
    wrapped = jnp.concatenate([fields[:, :, -1:], fields, fields[:, :, :1]], axis=2)
    return jnp.pad(wrapped, ((0, 0), (1, 1), (0, 0)))

def shifted(padded, offset, row_count, col_count):
    row_shift = offset // 3
    col_shift = offset % 3
    window = padded[:, row_shift:row_shift + row_count, col_shift:col_shift + col_count]
    return window.reshape(padded.shape[0], row_count * col_count)

def conv_forward(weights, padded, row_count, col_count):
    summed = None
    for offset in range(9):
        window = shifted(padded, offset, row_count, col_count)
        part = lax.dot_general(weights[offset], window, (((0,), (0,)), ((), ())), preferred_element_type=jnp.float32)
        summed = part if summed is None else summed + part
    return summed

def conv_back(weights, padded, row_count, col_count):
    summed = None
    for offset in range(9):
        window = shifted(padded, 8 - offset, row_count, col_count)
        part = jnp.dot(weights[offset], window, preferred_element_type=jnp.float32)
        summed = part if summed is None else summed + part
    return summed

def weight_grad(padded, deltas, row_count, col_count):
    parts = []
    for offset in range(9):
        window = shifted(padded, offset, row_count, col_count)
        parts.append(lax.dot_general(window, deltas, (((1,), (1,)), ((), ())), preferred_element_type=jnp.float32))
    return jnp.stack(parts)

def gelu_pair(pre):
    return jax.jvp(jax.nn.gelu, (pre,), (jnp.ones_like(pre),))

def noise_vectors(seeds):
    return (seeds.astype(jnp.float32) - 32767.5) / 18918.0

def combine(outputs, target_flat, weights, slope_sum, spread_sum, members):
    misses = outputs - target_flat[None]
    radius = jnp.sqrt(misses * misses + SMOOTH * SMOOTH)
    gradients = weights[None] * (misses / radius / members - slope_sum / (members * (members - 1)))
    loss_term = jnp.sum(weights[None] * ((radius - SMOOTH) / members - spread_sum / (2 * members * (members - 1))))
    return (gradients, loss_term)

def pair_sums(outputs, others):

    def add_member(running, member_out):
        gap_value = outputs - member_out.astype(jnp.float32)[None]
        radius = jnp.sqrt(gap_value * gap_value + SMOOTH * SMOOTH)
        return ((running[0] + gap_value / radius, running[1] + radius - SMOOTH), None)
    blank = jnp.zeros(outputs.shape, jnp.float32)
    sums, _ = lax.scan(add_member, (blank, blank), others)
    return sums

def member_forward(state, w_in, w_mid, w_out, noise_bias):
    row_count, col_count = (state.shape[1], state.shape[2])
    channels = w_in.shape[2]
    state_pad = pad_grid(state)
    pre_in = conv_forward(w_in, state_pad, row_count, col_count) + noise_bias[:, None]
    act_in, slope_in = gelu_pair(pre_in)
    hidden_in = act_in.astype(jnp.bfloat16)
    hidden_pad = pad_grid(hidden_in.reshape(channels, row_count, col_count))
    pre_mid = conv_forward(w_mid, hidden_pad, row_count, col_count)
    act_mid, slope_mid = gelu_pair(pre_mid)
    hidden_out = (act_mid + hidden_in.astype(jnp.float32)).astype(jnp.bfloat16)
    flat_state = state.reshape(state.shape[0], -1).astype(jnp.float32)
    output = (flat_state + jnp.dot(w_out, hidden_out, preferred_element_type=jnp.float32)).astype(jnp.bfloat16)
    return (state_pad, hidden_pad, hidden_out, slope_in, slope_mid, output)

def member_grads(state, w_in, w_mid, w_out, noise_bias, latent, delta_out):
    row_count, col_count = (state.shape[1], state.shape[2])
    channels = w_in.shape[2]
    state_pad, hidden_pad, hidden_out, slope_in, slope_mid, _ = member_forward(state, w_in, w_mid, w_out, noise_bias)
    grad_out = lax.dot_general(delta_out, hidden_out, (((1,), (1,)), ((), ())), preferred_element_type=jnp.float32)
    upstream = lax.dot_general(w_out, delta_out, (((0,), (0,)), ((), ())), preferred_element_type=jnp.float32)
    delta_mid = (upstream * slope_mid).astype(jnp.bfloat16)
    delta_pad = pad_grid(delta_mid.reshape(channels, row_count, col_count))
    incoming = conv_back(w_mid, delta_pad, row_count, col_count) + upstream
    delta_in = (incoming * slope_in).astype(jnp.bfloat16)
    grad_mid = weight_grad(hidden_pad, delta_mid, row_count, col_count)
    grad_in = weight_grad(state_pad, delta_in, row_count, col_count)
    grad_noise = latent[:, None] * lax.optimization_barrier(jnp.sum(delta_in.astype(jnp.float32), axis=1))[None, :]
    return (grad_in, grad_mid, grad_out, grad_noise)

def normalize(gradient):
    return gradient / jnp.sqrt(jnp.mean(gradient * gradient) + 1e-06)

def reference(state, target, land_sea, seeds, w_in, w_mid, w_out, w_noise):
    latents = noise_vectors(seeds)
    biases = jnp.dot(latents, w_noise, precision=lax.Precision.HIGHEST)
    members = seeds.shape[0]
    outputs = lax.map(lambda noise_bias: member_forward(state, w_in, w_mid, w_out, noise_bias)[5], biases)
    target_flat = target.reshape(target.shape[0], -1).astype(jnp.float32)
    weights = 1.0 + land_sea.reshape(1, -1).astype(jnp.float32)
    outputs_f = outputs.astype(jnp.float32)
    slope_sum, spread_sum = pair_sums(outputs_f, outputs)
    gradients, summed = combine(outputs_f, target_flat, weights, slope_sum, spread_sum, members)
    deltas = gradients.astype(jnp.bfloat16)
    grad_in, grad_mid, grad_out, grad_noise = lax.map(lambda packed: member_grads(state, w_in, w_mid, w_out, packed[0], packed[1], packed[2]), (biases, latents, deltas))
    loss = summed / (outputs.shape[1] * outputs.shape[2])
    return (normalize(lax.optimization_barrier(jnp.sum(grad_in, axis=0))), normalize(lax.optimization_barrier(jnp.sum(grad_mid, axis=0))), normalize(lax.optimization_barrier(jnp.sum(grad_out, axis=0))), normalize(lax.optimization_barrier(jnp.sum(grad_noise, axis=0))), loss)
```

```python
import jax
import jax.numpy as jnp
from jax import lax
from jax.experimental import pallas as pl
from jax.experimental.pallas import tpu as pltpu
from jax.sharding import PartitionSpec as P

SMOOTH = 0.25


MESH = pl.DeviceIdType.MESH
BLOCK = 8


def exchange(arrays, routes, cid):
    sent = len(routes)

    def kernel(*refs):
        ins = refs[: len(arrays)]
        outs = refs[len(arrays) : len(arrays) + sent]
        send_sem, recv_sem = refs[-2:]
        targets = []
        for _, shift in routes:
            targets.append(
                {
                    axis: lax.rem(lax.axis_index(axis) + by + lax.axis_size(axis), lax.axis_size(axis))
                    for axis, by in shift.items()
                }
            )
        barrier = pltpu.get_barrier_semaphore()
        for target in targets:
            pl.semaphore_signal(barrier, inc=1, device_id=target, device_id_type=MESH)
        pl.semaphore_wait(barrier, sent)
        copies = []
        for i, (k, _) in enumerate(routes):
            copy = pltpu.make_async_remote_copy(
                src_ref=ins[k],
                dst_ref=outs[i],
                send_sem=send_sem.at[i],
                recv_sem=recv_sem.at[i],
                device_id=targets[i],
                device_id_type=MESH,
            )
            copy.start()
            copies.append(copy)
        for copy in copies:
            copy.wait()

    vmem = pl.BlockSpec(memory_space=pltpu.VMEM)
    return pl.pallas_call(
        kernel,
        out_shape=[jax.ShapeDtypeStruct(arrays[k].shape, arrays[k].dtype) for k, _ in routes],
        in_specs=[vmem] * len(arrays),
        out_specs=[vmem] * sent,
        scratch_shapes=[pltpu.SemaphoreType.DMA((sent,)), pltpu.SemaphoreType.DMA((sent,))],
        compiler_params=pltpu.CompilerParams(collective_id=cid, has_side_effects=True),
        name=f"exchange_{cid}",
    )(*arrays)


def with_halo(block, cid):
    rows = block.shape[1]
    arrays = [block[:, rows - 1], block[:, 0], block[:, :, -1].T, block[:, :, 0].T]
    routes = [
        (0, {"lat": 1}),
        (1, {"lat": -1}),
        (2, {"lon": 1}),
        (3, {"lon": -1}),
        (2, {"lat": 1, "lon": 1}),
        (3, {"lat": 1, "lon": -1}),
        (2, {"lat": -1, "lon": 1}),
        (3, {"lat": -1, "lon": -1}),
    ]
    above, below, left, right, above_left, above_right, below_left, below_right = exchange(
        arrays, routes, cid
    )
    low = jnp.concatenate([above_left[rows - 1 :], left, below_left[:1]], axis=0).T
    high = jnp.concatenate([above_right[rows - 1 :], right, below_right[:1]], axis=0).T
    middle = jnp.concatenate([above[:, None], block, below[:, None]], axis=1)
    return jnp.concatenate([low[:, :, None], middle, high[:, :, None]], axis=2)


def reduce_groups():
    lat, lats = lax.axis_index("lat"), lax.axis_size("lat")
    cores = 2 if lats % 2 == 0 else 1
    core, row = lax.rem(lat, cores), lat // cores
    return {
        "core": (cores, core, lambda p: {"lat": row * cores + p}),
        "row": (lats // cores, row, lambda p: {"lat": p * cores + core}),
        "lon": (lax.axis_size("lon"), lax.axis_index("lon"), lambda p: {"lon": p}),
        "member": (lax.axis_size("member"), lax.axis_index("member"), lambda p: {"member": p}),
    }


ORDERS = (("core", "row", "lon", "member"), ("core", "lon", "row", "member"), ("core", "member", "row", "lon"))


def split_units(units):
    last = units // 7
    first = (units - last + 1) // 2
    return (first, units - last - first, last)


def sum_everywhere(array, cid):
    devices = lax.axis_size("lat") * lax.axis_size("lon") * lax.axis_size("member")
    rows = array.shape[0]
    unit = BLOCK * devices
    spans = []
    base = 0
    for order, units in zip(ORDERS, split_units(rows // unit)):
        if units:
            spans.append((order, base, units * unit))
            base += units * unit
    sizes = {
        "core": 2 if lax.axis_size("lat") % 2 == 0 else 1,
        "lon": lax.axis_size("lon"),
        "member": lax.axis_size("member"),
    }
    sizes["row"] = lax.axis_size("lat") // sizes["core"]
    plans = []
    landing = 0
    flags = 0
    for order, base, span in spans:
        steps = []
        for name in order:
            n = sizes[name]
            span //= n
            steps.append((name, n, span, landing, flags))
            landing += (n - 1) * span
            flags += n - 1
        plans.append((base, steps))
    stages = len(ORDERS[0])

    def kernel(in_ref, out_ref, held, landed, send_sem, recv_sem, send_back, recv_back):
        groups = reduce_groups()
        barrier = pltpu.get_barrier_semaphore()
        partners = 0
        for n, place, device in groups.values():
            for d in range(1, n):
                pl.semaphore_signal(
                    barrier, inc=1, device_id=device(lax.rem(place + d, n)), device_id_type=MESH
                )
                partners += 1
        pl.semaphore_wait(barrier, partners)
        starts = [[base] for base, _ in plans]
        for stage in range(stages):
            source = in_ref if stage == 0 else held
            target = out_ref if stage == stages - 1 else held
            running = []
            for p, (_, steps) in enumerate(plans):
                name, n, span, land, flag = steps[stage]
                _, place, device = groups[name]
                start = starts[p][-1]
                for d in range(1, n):
                    other = lax.rem(place + d, n)
                    copy = pltpu.make_async_remote_copy(
                        src_ref=source.at[pl.ds(pl.multiple_of(start + other * span, BLOCK), span)],
                        dst_ref=landed.at[pl.ds(land + (d - 1) * span, span)],
                        send_sem=send_sem.at[flag + d - 1],
                        recv_sem=recv_sem.at[flag + d - 1],
                        device_id=device(other),
                        device_id_type=MESH,
                    )
                    copy.start()
                    running.append((p, copy))
            for p, (_, steps) in enumerate(plans):
                name, n, span, land, flag = steps[stage]
                mine = starts[p][-1] + groups[name][1] * span
                starts[p].append(mine)
                for q, copy in running:
                    if q == p:
                        copy.wait()
                chunk = BLOCK
                while chunk < 64 and span % (2 * chunk) == 0:
                    chunk *= 2

                def add(i, carry, mine=mine, n=n, span=span, land=land, chunk=chunk):
                    at = pl.ds(pl.multiple_of(mine + i * chunk, BLOCK), chunk)
                    total = source[at]
                    for d in range(1, n):
                        total = total + landed[
                            pl.ds(pl.multiple_of(land + (d - 1) * span + i * chunk, BLOCK), chunk)
                        ]
                    target[at] = total
                    return carry

                lax.fori_loop(0, span // chunk, add, 0)
        for stage in reversed(range(stages)):
            running = []
            for p, (_, steps) in enumerate(plans):
                name, n, span, _, flag = steps[stage]
                _, place, device = groups[name]
                at = pl.ds(pl.multiple_of(starts[p][stage + 1], BLOCK), span)
                for d in range(1, n):
                    copy = pltpu.make_async_remote_copy(
                        src_ref=out_ref.at[at],
                        dst_ref=out_ref.at[at],
                        send_sem=send_back.at[flag + d - 1],
                        recv_sem=recv_back.at[flag + d - 1],
                        device_id=device(lax.rem(place + d, n)),
                        device_id_type=MESH,
                    )
                    copy.start()
                    running.append(copy)
            for copy in running:
                copy.wait()

    vmem = pl.BlockSpec(memory_space=pltpu.VMEM)
    dma = pltpu.SemaphoreType.DMA((flags,))
    return pl.pallas_call(
        kernel,
        out_shape=jax.ShapeDtypeStruct(array.shape, array.dtype),
        in_specs=[vmem],
        out_specs=vmem,
        scratch_shapes=[
            pltpu.VMEM(array.shape, array.dtype),
            pltpu.VMEM((landing, array.shape[1]), array.dtype),
            dma,
            dma,
            dma,
            dma,
        ],
        compiler_params=pltpu.CompilerParams(collective_id=cid, has_side_effects=True),
        name="sum_everywhere",
    )(array)


def sum_gradients(grad_in, grad_mid, grad_out, grad_noise, loss_term):
    devices = lax.axis_size("lat") * lax.axis_size("lon") * lax.axis_size("member")
    width = grad_in.shape[-1]
    parts = []
    places = []
    rows = 0
    for value in (grad_in, grad_mid, grad_out, grad_noise, jnp.full((1, width), loss_term)):
        short = -value.shape[-2] % BLOCK
        padded = jnp.pad(value, ((0, 0),) * (value.ndim - 2) + ((0, short), (0, 0)))
        flat = padded.reshape(-1, width)
        parts.append(flat)
        places.append((rows, flat.shape[0], padded.shape, value.shape[-2]))
        rows += flat.shape[0]
    parts.append(jnp.zeros((-rows % (BLOCK * devices), width), jnp.float32))
    summed = sum_everywhere(jnp.concatenate(parts, axis=0), 5)
    back = [
        summed[start : start + count].reshape(shape)[..., :real, :]
        for start, count, shape, real in places
    ]
    return (*back[:4], back[4][0, 0])


def shifted(padded, offset, row_count, col_count):
    row_shift = offset // 3
    col_shift = offset % 3
    window = padded[:, row_shift : row_shift + row_count, col_shift : col_shift + col_count]
    return window.reshape(padded.shape[0], row_count * col_count)


def conv_forward(weights, padded, row_count, col_count):
    summed = None
    for offset in range(9):
        window = shifted(padded, offset, row_count, col_count)
        part = lax.dot_general(
            weights[offset], window, (((0,), (0,)), ((), ())), preferred_element_type=jnp.float32
        )
        summed = part if summed is None else summed + part
    return summed


def conv_back(weights, padded, row_count, col_count):
    summed = None
    for offset in range(9):
        window = shifted(padded, 8 - offset, row_count, col_count)
        part = jnp.dot(weights[offset], window, preferred_element_type=jnp.float32)
        summed = part if summed is None else summed + part
    return summed


def weight_grad(padded, deltas, row_count, col_count):
    parts = []
    for offset in range(9):
        window = shifted(padded, offset, row_count, col_count)
        parts.append(
            lax.dot_general(
                window, deltas, (((1,), (1,)), ((), ())), preferred_element_type=jnp.float32
            )
        )
    return jnp.stack(parts)


def gelu_pair(pre):
    return jax.jvp(jax.nn.gelu, (pre,), (jnp.ones_like(pre),))


def clear_outside(padded, width, lat_index, lat_count):
    row_count = padded.shape[1] - 2 * width
    global_row = lat_index * row_count + jnp.arange(padded.shape[1], dtype=jnp.int32) - width
    inside = (global_row >= 0) & (global_row < row_count * lat_count)
    return jnp.where(inside[None, :, None], padded, jnp.zeros((), padded.dtype))


def combine(outputs, target_flat, weights, slope_sum, spread_sum, members):
    misses = outputs - target_flat[None]
    radius = jnp.sqrt(misses * misses + SMOOTH * SMOOTH)
    gradients = weights[None] * (misses / radius / members - slope_sum / (members * (members - 1)))
    loss_term = jnp.sum(
        weights[None] * ((radius - SMOOTH) / members - spread_sum / (2 * members * (members - 1)))
    )
    return (gradients, loss_term)


def pair_sums(outputs, others, running):
    slopes, spreads = running
    for member_out in others:
        gap_value = outputs - member_out.astype(jnp.float32)[None]
        radius = jnp.sqrt(gap_value * gap_value + SMOOTH * SMOOTH)
        slopes = slopes + gap_value / radius
        spreads = spreads + (radius - SMOOTH)
    return slopes, spreads


def normalize(gradient):
    return gradient / jnp.sqrt(jnp.mean(gradient * gradient) + 1e-06)


def body(state, target, land_sea, seeds, w_in, w_mid, w_out, w_noise):
    variables, row_count, col_count = state.shape
    channels = w_in.shape[2]
    cell_count = row_count * col_count
    lat_index = lax.axis_index("lat")
    lat_count = lax.axis_size("lat")
    members = lax.axis_size("member")
    latent = (seeds[0].astype(jnp.float32) - 32767.5) / 18918.0
    noise_bias = jnp.dot(latent, w_noise, precision=lax.Precision.HIGHEST)
    state_pad = with_halo(state, 1)
    state_pad = clear_outside(state_pad, 1, lat_index, lat_count)
    pre_in = conv_forward(w_in, state_pad, row_count, col_count) + noise_bias[:, None]
    act_in, slope_in = gelu_pair(pre_in)
    hidden_in = act_in.astype(jnp.bfloat16)
    hidden_pad = with_halo(hidden_in.reshape(channels, row_count, col_count), 2)
    hidden_pad = clear_outside(hidden_pad, 1, lat_index, lat_count)
    pre_mid = conv_forward(w_mid, hidden_pad, row_count, col_count)
    act_mid, slope_mid = gelu_pair(pre_mid)
    hidden_out = (act_mid + hidden_in.astype(jnp.float32)).astype(jnp.bfloat16)
    flat_state = state.reshape(variables, cell_count).astype(jnp.float32)
    output = (flat_state + jnp.dot(w_out, hidden_out, preferred_element_type=jnp.float32)).astype(
        jnp.bfloat16
    )
    target_flat = target.reshape(variables, cell_count).astype(jnp.float32)
    weights = 1.0 + land_sea.reshape(1, cell_count).astype(jnp.float32)
    own_output = output.astype(jnp.float32)[None]
    blank = jnp.zeros(own_output.shape, jnp.float32)
    others = exchange([output], [(0, {"member": d}) for d in range(1, members)], 4)
    slope_sum, spread_sum = pair_sums(own_output, [output, *others], (blank, blank))
    gradients, loss_term = combine(own_output, target_flat, weights, slope_sum, spread_sum, members)
    delta_out = gradients[0].astype(jnp.bfloat16)
    grad_out = lax.dot_general(
        delta_out, hidden_out, (((1,), (1,)), ((), ())), preferred_element_type=jnp.float32
    )
    upstream = lax.dot_general(
        w_out, delta_out, (((0,), (0,)), ((), ())), preferred_element_type=jnp.float32
    )
    delta_mid = (upstream * slope_mid).astype(jnp.bfloat16)
    delta_pad = with_halo(delta_mid.reshape(channels, row_count, col_count), 3)
    delta_pad = clear_outside(delta_pad, 1, lat_index, lat_count)
    incoming = conv_back(w_mid, delta_pad, row_count, col_count) + upstream
    delta_in = (incoming * slope_in).astype(jnp.bfloat16)
    grad_mid = weight_grad(hidden_pad, delta_mid, row_count, col_count)
    grad_in = weight_grad(state_pad, delta_in, row_count, col_count)
    grad_noise = latent[:, None] * jnp.sum(delta_in.astype(jnp.float32), axis=1)[None, :]
    grad_in, grad_mid, grad_out, grad_noise, summed = sum_gradients(
        grad_in, grad_mid, grad_out, grad_noise, loss_term
    )
    loss = summed / (variables * cell_count * lat_count * lax.axis_size("lon"))
    return (
        normalize(grad_in),
        normalize(grad_mid),
        normalize(grad_out),
        normalize(grad_noise),
        loss,
    )


def solution(mesh):
    placed = (
        P(None, "lat", "lon"),
        P(None, "lat", "lon"),
        P("lat", "lon"),
        P("member", None),
        P(),
        P(),
        P(),
        P(),
    )
    return jax.shard_map(
        body, mesh=mesh, in_specs=placed, out_specs=(P(), P(), P(), P(), P()), check_vma=False
    )
```
